32 devices in a mesh: ctx: 8 (over y, x, core), head: 4 (over z).
Axes of the slice: x: 2, y: 2, z: 4, core: 2. Of those that a mesh axis runs over, the one named last changes fastest.
Arguments:
- tokens: bfloat16 [1024, 4096], P('ctx'), may hold values from -8 to 8
- w_query: bfloat16 [4096, 4096], P(None, 'head'), may hold values from -1 to 1
- w_key: bfloat16 [4096, 1024], P(None, 'head'), may hold values from -1 to 1
- w_value: bfloat16 [4096, 1024], P(None, 'head'), may hold values from -0.09375 to 0.09375
- w_out: bfloat16 [4096, 4096], P('head'), may hold values from -0.09375 to 0.09375
- doc_ids: int32 [1024], P('ctx'), may hold values from 0 to 7, never falling along the last dimension, each value on 1 to 640 neighbouring positions
Outputs:
- mixed: bfloat16 [1024, 4096], P('ctx', 'head')
The draws below stay inside these ranges and needn't reach their ends.
Inputs may be any that keep to these rules, and one draw needn't show every extreme that they name: doc_ids never fall along the context; each document has 1 to 640 tokens and one has exactly 640.
All inputs are finite; a program needn't handle non-finite values.
Results may differ from the reference program's by a relative error of at most 0.011.
Values may be sent and summed in bfloat16 or wider, within the bound.
A program may use at most 128 MiB of HBM per device.

```python
import math
import jax
import jax.numpy as jnp
import numpy as np
from jax import lax

D = 4096
QH = 32
KVH = 8
HD = 128
TOKENS = 1024
DOC_MOST = 640
DOCS = 8
N_HEAD = 4


def drawn_weight(key, head_count, salt_value):
    entries = jax.random.truncated_normal(jax.random.fold_in(key, salt_value), -6.0, 6.0, (D, head_count * HD), jnp.float32) * D ** (-0.5)
    return entries.astype(jnp.bfloat16)


def draw_w_query(key, part):
    return drawn_weight(key, QH, 11)


def draw_w_key(key, part):
    return drawn_weight(key, KVH, 12)


def draw_tokens(key, part):
    values_drawn = jax.random.truncated_normal(jax.random.fold_in(key, 13), -6.0, 6.0, (TOKENS, D), jnp.float32)
    return values_drawn.astype(jnp.bfloat16)


def level_of(key, extent, shards, smallest, top_value):
    factor_of = 1.0
    for position, parts in shards:
        draws = jax.random.uniform(jax.random.fold_in(jax.random.fold_in(key, 6), position), (parts,), jnp.float32, smallest / len(shards), top_value / len(shards))
        factor_of = factor_of * jnp.repeat(jnp.exp(draws), extent[position] // parts).reshape((-1,) + (1,) * (len(extent) - 1 - position))
    return factor_of


def profile(amount, total, most, skew):
    loads = [(1 << 20) // math.isqrt(rank ** skew) + 1 for rank in range(2, amount + 1)]
    surplus, given = total - most - (amount - 1), [1] * (amount - 1)
    while surplus > 0:
        free = [i for i in range(amount - 1) if given[i] < most]
        whole, left = sum([loads[i] for i in free]), surplus
        for i in free:
            addition = min(most - given[i], max(1, left * loads[i] // whole), surplus)
            given[i] = given[i] + addition
            surplus = surplus - addition
    return np.array([most] + given)


def uneven_parts(key, count, total, bound, skew):
    if count == 2:
        one = jax.random.randint(key, (), max(1, total - bound), min(bound, total - 1) + 1)
        return jnp.stack([one, total - one])
    lengths = jnp.asarray(profile(count, total, bound, skew), jnp.int32)
    twos = (count - 1) // 2
    giver, taker = lengths[1:1 + 2 * twos:2], lengths[2:2 + 2 * twos:2]
    room = jnp.minimum(giver - 1, bound - taker)
    shifted = jax.random.randint(jax.random.fold_in(key, 1), (twos,), 0, 1 << 20) % (room + 1)
    lengths = lengths.at[1:1 + 2 * twos:2].set(giver - shifted).at[2:2 + 2 * twos:2].set(taker + shifted)
    return lengths[jax.random.permutation(jax.random.fold_in(key, 2), count)]


def scatter_about(own_key, extent, deviation, limit, pieces=(), kind=jnp.bfloat16):
    values = jax.random.normal(own_key, extent, jnp.float32) * deviation
    if len(pieces) > 0:
        values = level_of(own_key, extent, pieces, -0.22, 0.18) * values
    return jnp.clip(values, min=-limit, max=limit).astype(kind)


def setup_inputs(seed: int = 0) -> dict:
    key_of = jax.random.split(jax.random.key(seed), 7)
    return {
        "tokens": draw_tokens(jax.random.fold_in(key_of[6], 71), 0),
        "w_query": draw_w_query(jax.random.fold_in(key_of[6], 71), 0),
        "w_key": draw_w_key(jax.random.fold_in(key_of[6], 71), 0),
        "w_value": scatter_about(key_of[3], (D, KVH * HD), D ** -0.5, 0.09375, ((1, 4),)),
        "w_out": scatter_about(key_of[4], (QH * HD, D), (QH * HD) ** -0.5, 0.09375, ((0, 4),)),
        "doc_ids": jnp.searchsorted(jnp.cumsum(uneven_parts(key_of[5], DOCS, TOKENS, DOC_MOST, 2)), jnp.arange(TOKENS), side="right").astype(jnp.int32),
    }


def rotate(vectors, places):
    half_dim = vectors.shape[-1] // 2
    freqs = 500000.0 ** (-2.0 * jnp.arange(half_dim, dtype=jnp.float32) / vectors.shape[-1])
    angles = places.astype(jnp.float32)[:, None] * freqs[None, :]
    cosine = jnp.cos(angles)[:, None, :]
    sine = jnp.sin(angles)[:, None, :]
    first_half = vectors[..., :half_dim]
    second_half = vectors[..., half_dim:]
    return jnp.concatenate([first_half * cosine - second_half * sine, second_half * cosine + first_half * sine], axis=-1)

def reference(tokens, w_query, w_key, w_value, w_out, doc_ids):
    count = tokens.shape[0]
    places = jnp.arange(count, dtype=jnp.int32)
    queries = rotate(jnp.dot(tokens, w_query, preferred_element_type=jnp.float32).reshape(count, QH, HD), places).astype(jnp.bfloat16)
    keys_all = rotate(jnp.dot(tokens, w_key, preferred_element_type=jnp.float32).reshape(count, KVH, HD), places).astype(jnp.bfloat16)
    values_all = jnp.dot(tokens, w_value, preferred_element_type=jnp.float32).astype(jnp.bfloat16).reshape(count, KVH, HD)
    group_size = QH // KVH
    queries = queries.reshape(count, KVH, group_size, HD)
    block_rows = math.gcd(512, count)
    window = DOC_MOST + block_rows
    keys_pad = jnp.concatenate([jnp.zeros((DOC_MOST, KVH, HD), jnp.bfloat16), keys_all], axis=0)
    values_pad = jnp.concatenate([jnp.zeros((DOC_MOST, KVH, HD), jnp.bfloat16), values_all], axis=0)
    docs_pad = jnp.concatenate([jnp.full((DOC_MOST,), -1, jnp.int32), doc_ids], axis=0)
    score_scale = 1.0 / math.sqrt(HD)

    def one_block(block):
        q_start = (block * block_rows).astype(jnp.int32)
        q_block = lax.dynamic_slice_in_dim(queries, q_start, block_rows, 0).astype(jnp.float32)
        q_docs = lax.dynamic_slice_in_dim(doc_ids, q_start, block_rows, 0)
        q_index = q_start + jnp.arange(block_rows, dtype=jnp.int32)
        k_block = lax.dynamic_slice_in_dim(keys_pad, q_start, window, 0).astype(jnp.float32)
        v_block = lax.dynamic_slice_in_dim(values_pad, q_start, window, 0).astype(jnp.float32)
        k_docs = lax.dynamic_slice_in_dim(docs_pad, q_start, window, 0)
        k_index = q_start - DOC_MOST + jnp.arange(window, dtype=jnp.int32)
        allowed = (k_docs[None, :] == q_docs[:, None]) & (k_index[None, :] <= q_index[:, None])
        scores = jnp.einsum('tjgd,njd->jgtn', q_block, k_block) * score_scale
        scores = jnp.where(allowed, scores, -1e+30)
        top = lax.optimization_barrier(jnp.max(scores, axis=-1, keepdims=True))
        weights = jnp.exp(scores - top) * allowed.astype(jnp.float32)
        total = lax.optimization_barrier(jnp.sum(weights, axis=-1))
        summed = jnp.einsum('jgtn,njd->jgtd', weights.astype(jnp.bfloat16).astype(jnp.float32), v_block)
        result = summed / total[..., None]
        return jnp.transpose(result, (2, 0, 1, 3)).reshape(block_rows, QH * HD).astype(jnp.bfloat16)
    attended = lax.map(one_block, jnp.arange(count // block_rows, dtype=jnp.int32)).reshape(count, QH * HD)
    group_cols = QH * HD // N_HEAD
    mixed = jnp.zeros((count, D), jnp.float32)
    for group in range(N_HEAD):
        partial_value = jnp.dot(attended[:, group * group_cols:(group + 1) * group_cols], w_out[group * group_cols:(group + 1) * group_cols], preferred_element_type=jnp.float32).astype(jnp.bfloat16)
        partial_value = lax.optimization_barrier(partial_value)
        mixed = mixed + partial_value.astype(jnp.float32)
    return mixed.astype(jnp.bfloat16)
```

```python
import functools
import math

import jax
import jax.numpy as jnp
from jax import lax
from jax.experimental import pallas as pl
from jax.experimental.pallas import tpu as pltpu
from jax.sharding import PartitionSpec as P

HD = 128
BASE = 500000.0
STEPS = 4
SUB = 2
TAIL = 16
MESH = pl.DeviceIdType.MESH
FACTOR = math.log2(math.e) / math.sqrt(HD)


def kernel(
    n_ctx, n_head, reach,
    tokens, w_query, w_key, w_value, w_out, docs, out,
    tok, wq, wk, wv, wo, doc, kb, vb, q_acc, k_acc, v_acc, q, cos_ref, sin_ref, doc_q,
    top, tot, acc, att, part, rbuf,
    tok_sem, wk_sem, wv_sem, wq_sem, wo_sem, doc_sem,
    kv_send, kv_fwd, k_recv, v_recv, part_send, part_recv,
):
    rows = tokens.shape[0]
    kv_heads = w_key.shape[1] // HD
    heads = w_query.shape[1] // HD
    group = heads // kv_heads
    chips = n_ctx // 2
    near = (reach - 1) // 2
    me = lax.axis_index("ctx")
    z = lax.axis_index("head")
    core = lax.rem(me, 2)
    chip = me // 2
    partner = me + 1 - 2 * core
    step_rows = wq.shape[1]
    v_rows = wv.shape[1]
    piece = part.shape[2]

    def tok_copy(c):
        return pltpu.make_async_copy(
            tokens.at[:, c * step_rows:(c + 1) * step_rows], tok.at[c], tok_sem.at[c])

    def rows_copy(src, dst, sem, c):
        size = dst.shape[1]
        return pltpu.make_async_copy(src.at[c * size:(c + 1) * size, :], dst.at[c], sem.at[c])

    def wo_copy(t):
        width = SUB * piece
        return pltpu.make_async_copy(
            w_out.at[:, pl.ds(pl.multiple_of(t * width, width), width)], wo.at[t], wo_sem.at[t])

    def owner_of(k):
        return jnp.where(z < n_head // 2, n_head - 1 - k, k)

    doc_copy = pltpu.make_async_copy(docs, doc, doc_sem.at[0])
    doc_copy.start()
    for c in range(STEPS):
        tok_copy(c).start()
        rows_copy(w_key, wk, wk_sem, c).start()
    for c in range(STEPS // 2):
        rows_copy(w_value, wv, wv_sem, c).start()

    barrier = pltpu.get_barrier_semaphore()

    def greet(c, carry):
        @pl.when(c != chip)
        def _():
            pl.semaphore_signal(
                barrier, inc=1, device_id={"ctx": c * 2 + core}, device_id_type=MESH)
        return carry

    lax.fori_loop(0, chips, greet, 0)
    pl.semaphore_signal(barrier, inc=1, device_id={"ctx": partner}, device_id_type=MESH)
    gap = 2 * (near + 1) - 1

    @pl.when((core == 1) & (chip + near + 1 < chips))
    def _():
        pl.semaphore_signal(barrier, inc=1, device_id={"ctx": me + gap}, device_id_type=MESH)

    @pl.when((core == 0) & (chip > near))
    def _():
        pl.semaphore_signal(barrier, inc=1, device_id={"ctx": me - gap}, device_id_type=MESH)

    @pl.when(z > 0)
    def _():
        pl.semaphore_signal(barrier, inc=1, device_id={"head": z - 1}, device_id_type=MESH)

    @pl.when(z < n_head - 1)
    def _():
        pl.semaphore_signal(barrier, inc=1, device_id={"head": z + 1}, device_id_type=MESH)

    index = lax.broadcasted_iota(jnp.int32, (rows, HD), 1)
    freq = jnp.ones((rows, HD), jnp.float32)
    for b in range((HD // 2).bit_length() - 1):
        freq = freq * jnp.where(
            lax.rem(index // (1 << b), 2) == 1, jnp.float32(BASE ** (-2.0 * (1 << b) / HD)), 1.0)
    places = (me * rows + lax.broadcasted_iota(jnp.int32, (rows, HD), 0)).astype(jnp.float32)
    angles = places * freq
    cos_ref[...] = jnp.cos(angles)
    sine = jnp.sin(angles)
    sin_ref[...] = jnp.where(index < HD // 2, -sine, sine)

    def rotated(x):
        return (x * cos_ref[...] + pltpu.roll(x, HD // 2, 1) * sin_ref[...]).astype(jnp.bfloat16)

    for c in range(STEPS):
        tok_copy(c).wait()
        rows_copy(w_key, wk, wk_sem, c).wait()
        rows_copy(w_query, wq, wq_sem, c).start()
        product = jnp.dot(tok[c], wk[c], preferred_element_type=jnp.float32)
        k_acc[...] = product if c == 0 else k_acc[...] + product

    doc_copy.wait()
    doc_row = jnp.broadcast_to(doc[...].astype(jnp.float32), (rows, rows))
    doc_q[...] = doc_row.T
    kb[me, kv_heads * rows:, :] = doc_row[:TAIL].astype(jnp.bfloat16)
    for h in range(kv_heads):
        kb[me, h * rows:(h + 1) * rows, :] = rotated(k_acc[:, h * HD:(h + 1) * HD])

    pl.semaphore_wait(
        barrier,
        chips + (z > 0).astype(jnp.int32) + (z < n_head - 1).astype(jnp.int32)
        + ((core == 1) & (chip + near + 1 < chips)).astype(jnp.int32)
        + ((core == 0) & (chip > near)).astype(jnp.int32))

    def block_copy(ref, recv, send, block, target):
        return pltpu.make_async_remote_copy(
            src_ref=ref.at[block], dst_ref=ref.at[block],
            send_sem=send.at[0], recv_sem=recv.at[target - block - 1],
            device_id={"ctx": target}, device_id_type=MESH)

    def arrived(ref, recv, block):
        pltpu.make_async_remote_copy(
            src_ref=ref.at[block], dst_ref=ref.at[block],
            send_sem=kv_send.at[0], recv_sem=recv.at[me - block - 1],
            device_id={"ctx": partner}, device_id_type=MESH).wait_recv()

    last_near = jnp.minimum(chip + near, chips - 1)

    def own_targets(act):
        def one(c, carry):
            act(c * 2 + core)
            return carry

        lax.fori_loop(chip + 1, last_near + 1, one, 0)

        @pl.when(core == 0)
        def _():
            act(partner)

        @pl.when((core == 1) & (chip + near + 1 < chips))
        def _():
            act(me + gap)

    own_targets(lambda d: block_copy(kb, k_recv, kv_send, me, d).start())

    half = STEPS // 2
    for c in range(half):
        rows_copy(w_value, wv, wv_sem, c).wait()
        for i in range(STEPS // half):
            product = jnp.dot(
                tok[c * (STEPS // half) + i], wv[c, i * step_rows:(i + 1) * step_rows, :],
                preferred_element_type=jnp.float32)
            v_acc[...] = product if c == 0 and i == 0 else v_acc[...] + product
    vb[me] = v_acc[...].astype(jnp.bfloat16)
    own_targets(lambda d: block_copy(vb, v_recv, kv_send, me, d).start())

    for c in range(STEPS):
        rows_copy(w_query, wq, wq_sem, c).wait()
        if c < n_head:
            for k in range(c, n_head, STEPS):
                wo_copy(owner_of(k)).start()
        product = jnp.dot(tok[c], wq[c], preferred_element_type=jnp.float32)
        q_acc[...] = product if c == 0 else q_acc[...] + product
    for h in range(heads):
        q[h] = rotated(q_acc[:, h * HD:(h + 1) * HD])

    def block(j, own):
        ok = doc_q[...] == kb[j, kv_heads * rows:kv_heads * rows + 1, :].astype(jnp.float32)
        if own:
            ok = ok & (lax.broadcasted_iota(jnp.int32, (rows, rows), 1)
                       <= lax.broadcasted_iota(jnp.int32, (rows, rows), 0))
        bias = jnp.where(ok, 0.0, -1e30).astype(jnp.float32)
        for h in range(kv_heads):
            s = lax.dot_general(
                q[h * group:(h + 1) * group].reshape(group * rows, HD),
                kb[j, h * rows:(h + 1) * rows, :],
                (((1,), (1,)), ((), ())), preferred_element_type=jnp.float32)
            s = (s.reshape(group, rows, rows) + bias[None]).reshape(group * rows, rows)
            high = jnp.broadcast_to(jnp.max(s, axis=1, keepdims=True), s.shape)
            if not own:
                high = jnp.maximum(top[h], high)
                scale = jnp.exp2((top[h] - high) * FACTOR)
            p = jnp.exp2((s - high) * FACTOR)
            mixed = jnp.dot(
                p.astype(jnp.bfloat16), vb[j, :, h * HD:(h + 1) * HD],
                preferred_element_type=jnp.float32)
            top[h] = high
            tot[h] = p if own else tot[h] * scale + p
            acc[h] = mixed if own else acc[h] * scale + mixed

    block(me, True)

    @pl.when(core == 1)
    def _():
        arrived(kb, k_recv, me - 1)
        arrived(vb, v_recv, me - 1)
        block(me - 1, False)

    count = jnp.minimum(chip, near)

    def mine_of(i):
        return (chip - count + i) * 2 + core

    def other_of(i):
        return (chip - count + i) * 2 + 1 - core

    def pass_keys(i, carry):
        j = mine_of(i)
        arrived(kb, k_recv, j)

        block_copy(kb, k_recv, kv_fwd, j, partner).start()
        return carry

    lax.fori_loop(0, count, pass_keys, 0)

    def mine_step(i, carry):
        j = mine_of(i)
        arrived(vb, v_recv, j)
        block_copy(vb, v_recv, kv_fwd, j, partner).start()
        block(j, False)
        return carry

    lax.fori_loop(0, count, mine_step, 0)

    def other_step(i, carry):
        j = other_of(i)
        arrived(kb, k_recv, j)
        arrived(vb, v_recv, j)
        block(j, False)
        return carry

    lax.fori_loop(0, count, other_step, 0)

    @pl.when((core == 0) & (chip > near))
    def _():
        arrived(kb, k_recv, me - gap)
        arrived(vb, v_recv, me - gap)
        block(me - gap, False)

    for h in range(kv_heads):
        result = (acc[h] / jnp.sum(tot[h], axis=1, keepdims=True)).astype(jnp.bfloat16)
        for g in range(group):
            att[:, (h * group + g) * HD:(h * group + g + 1) * HD] = result[g * rows:(g + 1) * rows]

    def piece_copy(p, way):
        target = z + 1 if way == 0 else z - 1
        slot = p - SUB * target if way == 0 else SUB * (n_head - target) + p
        return pltpu.make_async_remote_copy(
            src_ref=part.at[p], dst_ref=rbuf.at[way, p],
            send_sem=part_send.at[0], recv_sem=part_recv.at[slot],
            device_id={"head": target}, device_id_type=MESH)

    def piece_arrived(p, way):
        slot = p - SUB * z if way == 0 else SUB * (n_head - z) + p
        pltpu.make_async_remote_copy(
            src_ref=part.at[p], dst_ref=rbuf.at[way, p],
            send_sem=part_send.at[0], recv_sem=part_recv.at[slot],
            device_id={"ctx": partner}, device_id_type=MESH).wait_recv()

    def project(k, carry):
        t = owner_of(k)
        wo_copy(t).wait()
        for s in range(SUB):
            p = t * SUB + s
            part[p] = jnp.dot(
                att[...], wo[t, :, s * piece:(s + 1) * piece],
                preferred_element_type=jnp.float32).astype(jnp.bfloat16)

            @pl.when((z == 0) & (t > 0))
            def _():
                piece_copy(p, 0).start()

            @pl.when((z == n_head - 1) & (t < n_head - 1))
            def _():
                piece_copy(p, 1).start()
        return carry

    lax.fori_loop(0, n_head, project, 0)

    def pass_on(p, way):
        piece_arrived(p, way)
        part[p] = (part[p].astype(jnp.float32) + rbuf[way, p].astype(jnp.float32)).astype(jnp.bfloat16)
        piece_copy(p, way).start()

    def relay(t, carry):
        a = t - z
        b = t - (n_head - 1 - z)

        @pl.when((z > 0) & (a >= 0) & (a < SUB * (n_head - 1 - z)))
        def _():
            pass_on((n_head - 1 - a // SUB) * SUB + lax.rem(a, SUB), 0)

        @pl.when((z < n_head - 1) & (b >= 0) & (b < SUB * z))
        def _():
            pass_on(b, 1)
        return carry

    @pl.when((z > 0) & (z < n_head - 1))
    def _():
        lax.fori_loop(0, SUB * (n_head - 1) + n_head, relay, 0)

    def last(s, add_left, add_right):
        p = z * SUB + s
        value = part[p].astype(jnp.float32)
        if add_left:
            piece_arrived(p, 0)
            value += rbuf[0, p].astype(jnp.float32)
        if add_right:
            piece_arrived(p, 1)
            value += rbuf[1, p].astype(jnp.float32)
        out[:, s * piece:(s + 1) * piece] = value.astype(jnp.bfloat16)

    own_targets(lambda d: block_copy(kb, k_recv, kv_send, me, d).wait_send())
    own_targets(lambda d: block_copy(vb, v_recv, kv_send, me, d).wait_send())

    def drain_forward(i, carry):
        block_copy(kb, k_recv, kv_fwd, mine_of(i), partner).wait_send()
        block_copy(vb, v_recv, kv_fwd, mine_of(i), partner).wait_send()
        return carry

    lax.fori_loop(0, count, drain_forward, 0)

    for which, left, right in ((z == 0, False, True), (z == n_head - 1, True, False),
                               ((z > 0) & (z < n_head - 1), True, True)):
        @pl.when(which)
        def _(left=left, right=right):
            for s in range(SUB):
                last(s, left, right)

    def drain_piece(p, carry):
        @pl.when((p < z * SUB) | (p >= (z + 1) * SUB))
        def _():
            pltpu.make_async_remote_copy(
                src_ref=part.at[p], dst_ref=rbuf.at[0, p],
                send_sem=part_send.at[0], recv_sem=part_recv.at[0],
                device_id={"ctx": partner}, device_id_type=MESH).wait_send()
        return carry

    lax.fori_loop(0, n_head * SUB, drain_piece, 0)


def solution(mesh):
    n_ctx, n_head = mesh.shape["ctx"], mesh.shape["head"]
    reach = n_ctx // 2 + 1

    def step(tokens, w_query, w_key, w_value, w_out, doc_ids):
        rows, width = tokens.shape
        q_width, kv_width = w_query.shape[1], w_key.shape[1]
        kv_heads, heads = kv_width // HD, q_width // HD
        group = heads // kv_heads
        step_rows = width // STEPS
        out_width = w_out.shape[1]
        pieces = n_head * SUB
        piece = out_width // pieces
        bf16, f32 = jnp.bfloat16, jnp.float32
        dma = pltpu.SemaphoreType.DMA
        return pl.pallas_call(
            functools.partial(kernel, n_ctx, n_head, reach),
            out_shape=pltpu.VMEM((rows, out_width // n_head), bf16),
            in_specs=[pl.BlockSpec(memory_space=pl.ANY)] * 6,
            out_specs=pl.BlockSpec(memory_space=pltpu.VMEM),
            scratch_shapes=[
                pltpu.VMEM((STEPS, rows, step_rows), bf16),
                pltpu.VMEM((STEPS, step_rows, q_width), bf16),
                pltpu.VMEM((STEPS, step_rows, kv_width), bf16),
                pltpu.VMEM((STEPS // 2, 2 * step_rows, kv_width), bf16),
                pltpu.VMEM((n_head, q_width, SUB * piece), bf16),
                pltpu.VMEM((1, rows), jnp.int32),
                pltpu.VMEM((n_ctx, kv_heads * rows + TAIL, HD), bf16),
                pltpu.VMEM((n_ctx, rows, kv_width), bf16),
                pltpu.VMEM((rows, q_width), f32),
                pltpu.VMEM((rows, kv_width), f32),
                pltpu.VMEM((rows, kv_width), f32),
                pltpu.VMEM((heads, rows, HD), bf16),
                pltpu.VMEM((rows, HD), f32),
                pltpu.VMEM((rows, HD), f32),
                pltpu.VMEM((rows, rows), f32),
                pltpu.VMEM((kv_heads, group * rows, rows), f32),
                pltpu.VMEM((kv_heads, group * rows, rows), f32),
                pltpu.VMEM((kv_heads, group * rows, HD), f32),
                pltpu.VMEM((rows, q_width), bf16),
                pltpu.VMEM((pieces, rows, piece), bf16),
                pltpu.VMEM((2, pieces, rows, piece), bf16),
                dma((STEPS,)), dma((STEPS,)), dma((STEPS // 2,)), dma((STEPS,)), dma((n_head,)), dma((1,)),
                dma((1,)), dma((1,)), dma((reach,)), dma((reach,)),
                dma((1,)), dma((SUB * (n_head + 1),)),
            ],
            compiler_params=pltpu.CompilerParams(
                collective_id=0, has_side_effects=True, vmem_limit_bytes=60 * 1024 * 1024),
            name="attention_layer",
        )(tokens, w_query, w_key, w_value, w_out, doc_ids.reshape(1, rows))

    return jax.shard_map(
        step,
        mesh=mesh,
        in_specs=(
            P("ctx", None),
            P(None, "head"),
            P(None, "head"),
            P(None, "head"),
            P("head", None),
            P("ctx"),
        ),
        out_specs=P("ctx", "head"),
        check_vma=False,
    )
```

```python
import functools
import math

import jax
import jax.numpy as jnp
from jax import lax
from jax.experimental import pallas as pl
from jax.experimental.pallas import tpu as pltpu
from jax.sharding import PartitionSpec as P

HD = 128
BASE = 500000.0
STEPS = 4
SUB = 4
SIDE = 2
WIDE = 2
TAIL = 16
MESH = pl.DeviceIdType.MESH
FACTOR = math.log2(math.e) / math.sqrt(HD)


def kernel(
    n_ctx, n_head, reach,
    tokens, w_query, w_key, w_value, w_out, docs, out,
    tok, wq, wk, wv, wo, doc, kb, vb, q_acc, k_acc, v_acc, q, cos_ref, sin_ref,
    top, tot, acc, att, part, rbuf, side,
    tok_sem, wk_sem, wv_sem, wq_sem, wo_sem, doc_sem,
    kv_send, kv_fwd, k_recv, v_recv, part_send, part_recv, side_recv,
):
    rows = tokens.shape[0]
    kv_heads = w_key.shape[1] // HD
    heads = w_query.shape[1] // HD
    group = heads // kv_heads
    chips = n_ctx // 2
    near = (reach - 1) // 2
    me = lax.axis_index("ctx")
    z = lax.axis_index("head")
    core = lax.rem(me, 2)
    chip = me // 2
    partner = me + 1 - 2 * core
    step_rows = wq.shape[1]
    v_rows = wv.shape[1]
    piece = part.shape[2]

    def tok_copy(c):
        return pltpu.make_async_copy(
            tokens.at[:, c * step_rows:(c + 1) * step_rows], tok.at[c], tok_sem.at[c])

    def rows_copy(src, dst, sem, c):
        size = dst.shape[1]
        return pltpu.make_async_copy(src.at[c * size:(c + 1) * size, :], dst.at[c], sem.at[c])

    def wo_copy(t):
        width = SUB * piece
        return pltpu.make_async_copy(
            w_out.at[:, pl.ds(pl.multiple_of(t * width, width), width)], wo.at[t], wo_sem.at[t])

    def owner_of(k):
        return jnp.where(z < n_head // 2, n_head - 1 - k, k)

    doc_copy = pltpu.make_async_copy(docs, doc, doc_sem.at[0])
    doc_copy.start()
    for c in range(STEPS):
        tok_copy(c).start()
        rows_copy(w_key, wk, wk_sem, c).start()

    barrier = pltpu.get_barrier_semaphore()

    def greet(c, carry):
        @pl.when(c != chip)
        def _():
            pl.semaphore_signal(
                barrier, inc=1, device_id={"ctx": c * 2 + core}, device_id_type=MESH)
        return carry

    lax.fori_loop(0, chips, greet, 0)
    pl.semaphore_signal(barrier, inc=1, device_id={"ctx": partner}, device_id_type=MESH)
    gap = 2 * (near + 1) - 1
    detour = chips == 4 and n_head == 4
    helper, giver = chip == 0, chip == 2
    greeted = chips + (z > 0).astype(jnp.int32) + (z < n_head - 1).astype(jnp.int32)
    if detour:
        for inner, edge in ((1, 0), (n_head - 2, n_head - 1)):
            @pl.when(giver & (z == inner))
            def _(edge=edge):
                pl.semaphore_signal(
                    barrier, inc=1, device_id={"ctx": me - n_ctx // 2, "head": edge},
                    device_id_type=MESH)

        greeted = greeted + (helper & ((z == 0) | (z == n_head - 1))).astype(jnp.int32)

    @pl.when((core == 1) & (chip + near + 1 < chips))
    def _():
        pl.semaphore_signal(barrier, inc=1, device_id={"ctx": me + gap}, device_id_type=MESH)

    @pl.when((core == 0) & (chip > near))
    def _():
        pl.semaphore_signal(barrier, inc=1, device_id={"ctx": me - gap}, device_id_type=MESH)

    @pl.when(z > 0)
    def _():
        pl.semaphore_signal(barrier, inc=1, device_id={"head": z - 1}, device_id_type=MESH)

    @pl.when(z < n_head - 1)
    def _():
        pl.semaphore_signal(barrier, inc=1, device_id={"head": z + 1}, device_id_type=MESH)

    index = lax.broadcasted_iota(jnp.int32, (rows, HD), 1)
    freq = jnp.ones((rows, HD), jnp.float32)
    for b in range((HD // 2).bit_length() - 1):
        freq = freq * jnp.where(
            lax.rem(index // (1 << b), 2) == 1, jnp.float32(BASE ** (-2.0 * (1 << b) / HD)), 1.0)
    places = (me * rows + lax.broadcasted_iota(jnp.int32, (rows, HD), 0)).astype(jnp.float32)
    angles = places * freq
    cos_ref[...] = jnp.cos(angles)
    sine = jnp.sin(angles)
    sin_ref[...] = jnp.where(index < HD // 2, -sine, sine)

    def rotated(x):
        return (x * cos_ref[...] + pltpu.roll(x, HD // 2, 1) * sin_ref[...]).astype(jnp.bfloat16)

    for c in range(STEPS):
        tok_copy(c).wait()
        rows_copy(w_key, wk, wk_sem, c).wait()
        if c < STEPS // 2:
            rows_copy(w_value, wv, wv_sem, c).start()
        else:
            for i in range(2 * c - STEPS, 2 * c - STEPS + 2):
                rows_copy(w_query, wq, wq_sem, i).start()
        product = jnp.dot(tok[c], wk[c], preferred_element_type=jnp.float32)
        k_acc[...] = product if c == 0 else k_acc[...] + product

    doc_copy.wait()
    kb[me, kv_heads * rows:, :] = jnp.broadcast_to(
        doc[...].astype(jnp.float32), (TAIL, rows)).astype(jnp.bfloat16)
    for h in range(kv_heads):
        kb[me, h * rows:(h + 1) * rows, :] = rotated(k_acc[:, h * HD:(h + 1) * HD])

    pl.semaphore_wait(
        barrier,
        greeted + ((core == 1) & (chip + near + 1 < chips)).astype(jnp.int32)
        + ((core == 0) & (chip > near)).astype(jnp.int32))

    def block_copy(ref, recv, send, block, target):
        return pltpu.make_async_remote_copy(
            src_ref=ref.at[block], dst_ref=ref.at[block],
            send_sem=send.at[0], recv_sem=recv.at[target - block - 1],
            device_id={"ctx": target}, device_id_type=MESH)

    def arrived(ref, recv, block):
        pltpu.make_async_remote_copy(
            src_ref=ref.at[block], dst_ref=ref.at[block],
            send_sem=kv_send.at[0], recv_sem=recv.at[me - block - 1],
            device_id={"ctx": partner}, device_id_type=MESH).wait_recv()

    last_near = jnp.minimum(chip + near, chips - 1)

    relayed = ((chip == 1) & (core == 1)).astype(jnp.int32)
    bearer = (chip == 3) & (core == 1)

    def own_targets(act):
        def one(c, carry):
            act(c * 2 + core)
            return carry

        if detour:
            lax.fori_loop(chip + 1, last_near + 1 - 2 * relayed, one, 0)

            @pl.when(relayed == 1)
            def _():
                act(me + 4)
        else:
            lax.fori_loop(chip + 1, last_near + 1, one, 0)

        @pl.when(core == 0)
        def _():
            act(partner)

        @pl.when((core == 1) & (chip + near + 1 < chips))
        def _():
            act(me + gap)

    own_targets(lambda d: block_copy(kb, k_recv, kv_send, me, d).start())

    half = STEPS // 2
    for c in range(half):
        rows_copy(w_value, wv, wv_sem, c).wait()
        for i in range(STEPS // half):
            product = jnp.dot(
                tok[c * (STEPS // half) + i], wv[c, i * step_rows:(i + 1) * step_rows, :],
                preferred_element_type=jnp.float32)
            v_acc[...] = product if c == 0 and i == 0 else v_acc[...] + product
    for h in range(kv_heads):
        vb[me, h * HD:(h + 1) * HD, :] = v_acc[:, h * HD:(h + 1) * HD].T.astype(jnp.bfloat16)
    own_targets(lambda d: block_copy(vb, v_recv, kv_send, me, d).start())

    for c in range(STEPS):
        rows_copy(w_query, wq, wq_sem, c).wait()
        if c < n_head:
            for k in range(c, n_head, STEPS):
                wo_copy(owner_of(k)).start()
        product = jnp.dot(tok[c], wq[c], preferred_element_type=jnp.float32)
        q_acc[...] = product if c == 0 else q_acc[...] + product
    for h in range(heads):
        g = h % group
        q[h // group, g * rows:(g + 1) * rows, :] = rotated(q_acc[:, h * HD:(h + 1) * HD])

    def attend(js, own, ready=None):
        doc_row = doc[...].astype(jnp.float32)
        biases = []
        for i, j in enumerate(js):
            column = kb[j, kv_heads * rows:kv_heads * rows + 1, :].astype(jnp.float32)
            ok = jnp.broadcast_to(column, (rows, rows)).T == doc_row
            if own and i == 0:
                ok = ok & (lax.broadcasted_iota(jnp.int32, (rows, rows), 0)
                           <= lax.broadcasted_iota(jnp.int32, (rows, rows), 1))
            bias = jnp.where(ok, 0.0, -1e30).astype(jnp.float32)
            biases.append(jnp.concatenate([bias] * group, axis=1))
        scores = [
            [bias + lax.dot_general(
                kb[j, h * rows:(h + 1) * rows, :], q[h],
                (((1,), (1,)), ((), ())), preferred_element_type=jnp.float32)
             for j, bias in zip(js, biases)]
            for h in range(kv_heads)]
        scales, weights = [], []
        for h in range(kv_heads):
            high = jnp.max(functools.reduce(jnp.maximum, scores[h]), axis=0, keepdims=True)
            if not own:
                high = jnp.maximum(top[h], high)
                scales.append(jnp.exp2((top[h] - high) * FACTOR))
            ps = [jnp.exp2((s - high) * FACTOR) for s in scores[h]]
            total = jnp.sum(functools.reduce(jnp.add, ps), axis=0, keepdims=True)
            top[h] = high
            tot[h] = total if own else tot[h] * scales[h] + total
            weights.append(jnp.concatenate([p.astype(jnp.bfloat16) for p in ps], axis=0))
        if ready is not None:
            ready()
        for h in range(kv_heads):
            mixed = jnp.dot(
                jnp.concatenate([vb[j, h * HD:(h + 1) * HD, :] for j in js], axis=1),
                weights[h], preferred_element_type=jnp.float32)
            acc[h] = mixed if own else acc[h] * scales[h] + mixed

    def keys_in(j):
        arrived(kb, k_recv, j)

    def values_in(j):
        arrived(vb, v_recv, j)

    def pass_on_block(ref, recv, j, relays):
        block_copy(ref, recv, kv_fwd, j, partner).start()
        if relays:
            @pl.when(bearer)
            def _():
                block_copy(ref, recv, kv_fwd, j, me - 2).start()

    def keys_on(j, relays=False):
        keys_in(j)
        pass_on_block(kb, k_recv, j, relays)

    def values_on(j, relays=False):
        values_in(j)
        pass_on_block(vb, v_recv, j, relays)

    @pl.when(core == 0)
    def _():
        attend([me], True)

    @pl.when(core == 1)
    def _():
        keys_in(me - 1)
        attend([me, me - 1], True, lambda: values_in(me - 1))

    count = jnp.minimum(chip, near)

    def mine_of(i):
        return (chip - count + i) * 2 + core

    def other_of(i):
        return (chip - count + i) * 2 + 1 - core

    def chip_step(i, carry):
        mine, other = mine_of(i), other_of(i)
        keys_on(mine)
        attend([mine], False, lambda: values_on(mine))
        keys_in(other)
        attend([other], False, lambda: values_in(other))
        return carry

    def far_step(js):
        for j in js:
            keys_in(j)

        def ready():
            for j in js:
                values_in(j)

        attend(js, False, ready)

    if near == 2:
        @pl.when(chip <= near)
        def _():
            lax.fori_loop(0, count, chip_step, 0)

        @pl.when(chip > near)
        def _():
            mine, other = [mine_of(0), mine_of(1)], [other_of(0), other_of(1)]
            for i, j in enumerate(mine):
                keys_on(j, detour and i == 0)

            def ready():
                for i, j in enumerate(mine):
                    values_on(j, detour and i == 0)

            attend(mine, False, ready)

            @pl.when(core == 0)
            def _():
                far_step(other + [me - gap])

            @pl.when(core == 1)
            def _():
                far_step(other)
    else:
        lax.fori_loop(0, count, chip_step, 0)

        @pl.when((core == 0) & (chip > near))
        def _():
            far_step([me - gap])

    for h in range(kv_heads):
        result = acc[h] * (1.0 / tot[h])
        for g in range(group):
            att[:, (h * group + g) * HD:(h * group + g + 1) * HD] = (
                result[:, g * rows:(g + 1) * rows].T.astype(jnp.bfloat16))

    def piece_copy(p, way, source=None, ctx=None):
        target = z + 1 if way == 0 else z - 1
        slot = p - SUB * target if way == 0 else SUB * (n_head - target) + p
        return pltpu.make_async_remote_copy(
            src_ref=part.at[p] if source is None else source, dst_ref=rbuf.at[way, p],
            send_sem=part_send.at[0], recv_sem=part_recv.at[slot],
            device_id={"head": target} if ctx is None else {"ctx": ctx, "head": target},
            device_id_type=MESH)

    def side_copy(p, i, ctx):
        return pltpu.make_async_remote_copy(
            src_ref=part.at[p], dst_ref=side.at[i],
            send_sem=part_send.at[0], recv_sem=side_recv.at[i],
            device_id={"ctx": ctx}, device_id_type=MESH)

    def piece_arrived(p, way):
        slot = p - SUB * z if way == 0 else SUB * (n_head - z) + p
        pltpu.make_async_remote_copy(
            src_ref=part.at[p], dst_ref=rbuf.at[way, p],
            send_sem=part_send.at[0], recv_sem=part_recv.at[slot],
            device_id={"ctx": partner}, device_id_type=MESH).wait_recv()

    def project(k, carry):
        t = owner_of(k)
        wo_copy(t).wait()
        for s in range(SUB):
            p = t * SUB + s
            if s % WIDE == 0:
                product = jnp.dot(
                    att[...], wo[t, :, s * piece:(s + WIDE) * piece],
                    preferred_element_type=jnp.float32).astype(jnp.bfloat16)
                for i in range(WIDE):
                    part[p + i] = product[:, i * piece:(i + 1) * piece]

            def send(way, t=t, p=p, s=s):
                if not detour:
                    piece_copy(p, way).start()
                    return
                nearest = t == (1 if way == 0 else n_head - 2)
                given, held = nearest & giver & (s < SIDE), nearest & helper & (s >= SUB - SIDE)

                @pl.when(jnp.logical_not(given | held))
                def _():
                    piece_copy(p, way).start()

                if s < SIDE:
                    @pl.when(given)
                    def _():
                        side_copy(p, s, me - n_ctx // 2).start()

            @pl.when((z == 0) & (t > 0))
            def _(send=send):
                send(0)

            @pl.when((z == n_head - 1) & (t < n_head - 1))
            def _(send=send):
                send(1)
        return carry

    lax.fori_loop(0, n_head, project, 0)

    if detour:
        for edge, way, t in ((0, 0, 1), (n_head - 1, 1, n_head - 2)):
            @pl.when(helper & (z == edge))
            def _(way=way, t=t):
                for i in range(SIDE):
                    side_copy(t * SUB + i, i, partner).wait_recv()
                    piece_copy(t * SUB + i, way, side.at[i], me + n_ctx // 2).start()
                for i in range(SUB - SIDE, SUB):
                    piece_copy(t * SUB + i, way).start()

    def pass_on(p, way):
        piece_arrived(p, way)
        part[p] = (part[p].astype(jnp.float32) + rbuf[way, p].astype(jnp.float32)).astype(jnp.bfloat16)
        piece_copy(p, way).start()

    def relay(t, carry):
        a = t - (SUB - 1) * z
        b = t - (SUB - 1) * (n_head - 1 - z)

        @pl.when((z > 0) & (a >= 0) & (a < SUB * (n_head - 1 - z)))
        def _():
            pass_on((n_head - 1 - a // SUB) * SUB + lax.rem(a, SUB), 0)

        @pl.when((z < n_head - 1) & (b >= 0) & (b < SUB * z))
        def _():
            pass_on(b, 1)
        return carry

    @pl.when((z > 0) & (z < n_head - 1))
    def _():
        lax.fori_loop(0, (2 * SUB - 1) * (n_head - 1), relay, 0)

    def last(s, add_left, add_right):
        p = z * SUB + s
        value = part[p].astype(jnp.float32)
        if add_left:
            piece_arrived(p, 0)
            value += rbuf[0, p].astype(jnp.float32)
        if add_right:
            piece_arrived(p, 1)
            value += rbuf[1, p].astype(jnp.float32)
        out[:, s * piece:(s + 1) * piece] = value.astype(jnp.bfloat16)

    own_targets(lambda d: block_copy(kb, k_recv, kv_send, me, d).wait_send())
    own_targets(lambda d: block_copy(vb, v_recv, kv_send, me, d).wait_send())

    def drain_forward(i, carry):
        block_copy(kb, k_recv, kv_fwd, mine_of(i), partner).wait_send()
        block_copy(vb, v_recv, kv_fwd, mine_of(i), partner).wait_send()
        return carry

    lax.fori_loop(0, count, drain_forward, 0)
    if detour:
        @pl.when(bearer)
        def _():
            drain_forward(0, 0)

    for which, left, right in ((z == 0, False, True), (z == n_head - 1, True, False),
                               ((z > 0) & (z < n_head - 1), True, True)):
        @pl.when(which)
        def _(left=left, right=right):
            for s in range(SUB):
                last(s, left, right)

    def drain_piece(p, carry):
        @pl.when((p < z * SUB) | (p >= (z + 1) * SUB))
        def _():
            pltpu.make_async_remote_copy(
                src_ref=part.at[p], dst_ref=rbuf.at[0, p],
                send_sem=part_send.at[0], recv_sem=part_recv.at[0],
                device_id={"ctx": partner}, device_id_type=MESH).wait_send()
        return carry

    lax.fori_loop(0, n_head * SUB, drain_piece, 0)

    if detour:
        @pl.when(helper & ((z == 0) | (z == n_head - 1)))
        def _():
            for i in range(SIDE):
                side_copy(0, i, partner).wait_send()


def solution(mesh):
    n_ctx, n_head = mesh.shape["ctx"], mesh.shape["head"]
    reach = n_ctx // 2 + 1

    def step(tokens, w_query, w_key, w_value, w_out, doc_ids):
        rows, width = tokens.shape
        q_width, kv_width = w_query.shape[1], w_key.shape[1]
        kv_heads, heads = kv_width // HD, q_width // HD
        group = heads // kv_heads
        step_rows = width // STEPS
        out_width = w_out.shape[1]
        pieces = n_head * SUB
        piece = out_width // pieces
        bf16, f32 = jnp.bfloat16, jnp.float32
        dma = pltpu.SemaphoreType.DMA
        return pl.pallas_call(
            functools.partial(kernel, n_ctx, n_head, reach),
            out_shape=pltpu.VMEM((rows, out_width // n_head), bf16),
            in_specs=[pl.BlockSpec(memory_space=pl.ANY)] * 6,
            out_specs=pl.BlockSpec(memory_space=pltpu.VMEM),
            scratch_shapes=[
                pltpu.VMEM((STEPS, rows, step_rows), bf16),
                pltpu.VMEM((STEPS, step_rows, q_width), bf16),
                pltpu.VMEM((STEPS, step_rows, kv_width), bf16),
                pltpu.VMEM((STEPS // 2, 2 * step_rows, kv_width), bf16),
                pltpu.VMEM((n_head, q_width, SUB * piece), bf16),
                pltpu.VMEM((1, rows), jnp.int32),
                pltpu.VMEM((n_ctx, kv_heads * rows + TAIL, HD), bf16),
                pltpu.VMEM((n_ctx, kv_width, rows), bf16),
                pltpu.VMEM((rows, q_width), f32),
                pltpu.VMEM((rows, kv_width), f32),
                pltpu.VMEM((rows, kv_width), f32),
                pltpu.VMEM((kv_heads, group * rows, HD), bf16),
                pltpu.VMEM((rows, HD), f32),
                pltpu.VMEM((rows, HD), f32),
                pltpu.VMEM((kv_heads, 1, group * rows), f32),
                pltpu.VMEM((kv_heads, 1, group * rows), f32),
                pltpu.VMEM((kv_heads, HD, group * rows), f32),
                pltpu.VMEM((rows, q_width), bf16),
                pltpu.VMEM((pieces, rows, piece), bf16),
                pltpu.VMEM((2, pieces, rows, piece), bf16),
                pltpu.VMEM((SIDE, rows, piece), bf16),
                dma((STEPS,)), dma((STEPS,)), dma((STEPS // 2,)), dma((STEPS,)), dma((n_head,)), dma((1,)),
                dma((1,)), dma((1,)), dma((reach,)), dma((reach,)),
                dma((1,)), dma((SUB * (n_head + 1),)), dma((SIDE,)),
            ],
            compiler_params=pltpu.CompilerParams(
                collective_id=0, has_side_effects=True, vmem_limit_bytes=60 * 1024 * 1024),
            name="attention_layer",
        )(tokens, w_query, w_key, w_value, w_out, doc_ids.reshape(1, rows))

    return jax.shard_map(
        step,
        mesh=mesh,
        in_specs=(
            P("ctx", None),
            P(None, "head"),
            P(None, "head"),
            P(None, "head"),
            P("head", None),
            P("ctx"),
        ),
        out_specs=P("ctx", "head"),
        check_vma=False,
    )
```

```python
import functools
import math

import jax
import jax.numpy as jnp
from jax import lax
from jax.experimental import pallas as pl
from jax.experimental.pallas import tpu as pltpu
from jax.sharding import PartitionSpec as P

HD = 128
BASE = 500000.0
STEPS = 4
SUB = 4
SIDE = 2
WIDE = 2
TAIL = 16
MESH = pl.DeviceIdType.MESH
FACTOR = math.log2(math.e) / math.sqrt(HD)


def kernel(
    n_ctx, n_head, reach,
    tokens, w_query, w_key, w_value, w_out, docs, out,
    tok, wq, wk, wv, wo, doc, kb, vb, q_acc, k_acc, v_acc, q, cos_ref, sin_ref,
    top, tot, acc, att, part, rbuf, side,
    wq_sem, wo_sem, wv_sem, doc_sem,
    kv_send, kv_fwd, k_recv, v_recv, part_send, part_recv, side_recv,
):
    rows = tokens.shape[0]
    kv_heads = w_key.shape[1] // HD
    heads = w_query.shape[1] // HD
    group = heads // kv_heads
    chips = n_ctx // 2
    near = (reach - 1) // 2
    me = lax.axis_index("ctx")
    z = lax.axis_index("head")
    core = lax.rem(me, 2)
    chip = me // 2
    partner = me + 1 - 2 * core
    step_rows = wq.shape[1]
    v_rows = wv.shape[1]
    piece = part.shape[2]

    def tok_copy(c):
        return pltpu.make_async_copy(
            tokens.at[:, c * step_rows:(c + 1) * step_rows], tok.at[c], wq_sem.at[c])

    def rows_copy(src, dst, sem, c):
        size = dst.shape[1]
        return pltpu.make_async_copy(src.at[c * size:(c + 1) * size, :], dst.at[c], sem.at[c])

    def wo_copy(t):
        width = SUB * piece
        return pltpu.make_async_copy(
            w_out.at[:, pl.ds(pl.multiple_of(t * width, width), width)], wo.at[t], wo_sem.at[t])

    def owner_of(k):
        return jnp.where(z < n_head // 2, n_head - 1 - k, k)

    doc_copy = pltpu.make_async_copy(docs, doc, doc_sem.at[0])
    doc_copy.start()
    for c in range(STEPS):
        tok_copy(c).start()
        rows_copy(w_key, wk, wo_sem, c).start()

    barrier = pltpu.get_barrier_semaphore()

    def greet(c, carry):
        @pl.when(c != chip)
        def _():
            pl.semaphore_signal(
                barrier, inc=1, device_id={"ctx": c * 2 + core}, device_id_type=MESH)
        return carry

    lax.fori_loop(0, chips, greet, 0)
    pl.semaphore_signal(barrier, inc=1, device_id={"ctx": partner}, device_id_type=MESH)
    gap = 2 * (near + 1) - 1
    detour = chips == 4 and n_head == 4
    helper, giver = chip == 0, chip == 2
    greeted = chips + (z > 0).astype(jnp.int32) + (z < n_head - 1).astype(jnp.int32)
    if detour:
        for inner, edge in ((1, 0), (n_head - 2, n_head - 1)):
            @pl.when(giver & (z == inner))
            def _(edge=edge):
                pl.semaphore_signal(
                    barrier, inc=1, device_id={"ctx": me - n_ctx // 2, "head": edge},
                    device_id_type=MESH)

        greeted = greeted + (helper & ((z == 0) | (z == n_head - 1))).astype(jnp.int32)

    @pl.when((core == 1) & (chip + near + 1 < chips))
    def _():
        pl.semaphore_signal(barrier, inc=1, device_id={"ctx": me + gap}, device_id_type=MESH)

    @pl.when((core == 0) & (chip > near))
    def _():
        pl.semaphore_signal(barrier, inc=1, device_id={"ctx": me - gap}, device_id_type=MESH)

    @pl.when(z > 0)
    def _():
        pl.semaphore_signal(barrier, inc=1, device_id={"head": z - 1}, device_id_type=MESH)

    @pl.when(z < n_head - 1)
    def _():
        pl.semaphore_signal(barrier, inc=1, device_id={"head": z + 1}, device_id_type=MESH)

    index = lax.broadcasted_iota(jnp.int32, (rows, HD), 1)
    freq = jnp.ones((rows, HD), jnp.float32)
    for b in range((HD // 2).bit_length() - 1):
        freq = freq * jnp.where(
            lax.rem(index // (1 << b), 2) == 1, jnp.float32(BASE ** (-2.0 * (1 << b) / HD)), 1.0)
    places = (me * rows + lax.broadcasted_iota(jnp.int32, (rows, HD), 0)).astype(jnp.float32)
    angles = places * freq
    cos_ref[...] = jnp.cos(angles)
    sine = jnp.sin(angles)
    sin_ref[...] = jnp.where(index < HD // 2, -sine, sine)

    rows_copy(w_value, wv, wv_sem, 0).start()

    def rotated(x):
        return (x * cos_ref[...] + pltpu.roll(x, HD // 2, 1) * sin_ref[...]).astype(jnp.bfloat16)

    for c in range(STEPS):
        tok_copy(c).wait()
        rows_copy(w_key, wk, wo_sem, c).wait()
        for i in ((), (0,), (1,), (2, 3))[c]:
            rows_copy(w_query, wq, wq_sem, i).start()
        if c == 0:
            rows_copy(w_value, wv, wv_sem, 1).start()
        product = jnp.dot(tok[c], wk[c], preferred_element_type=jnp.float32)
        k_acc[...] = product if c == 0 else k_acc[...] + product

    doc_copy.wait()
    kb[me, kv_heads * rows:, :] = jnp.broadcast_to(
        doc[...].astype(jnp.float32), (TAIL, rows)).astype(jnp.bfloat16)
    for h in range(kv_heads):
        kb[me, h * rows:(h + 1) * rows, :] = rotated(k_acc[:, h * HD:(h + 1) * HD])

    pl.semaphore_wait(
        barrier,
        greeted + ((core == 1) & (chip + near + 1 < chips)).astype(jnp.int32)
        + ((core == 0) & (chip > near)).astype(jnp.int32))

    def block_copy(ref, recv, send, block, target):
        return pltpu.make_async_remote_copy(
            src_ref=ref.at[block], dst_ref=ref.at[block],
            send_sem=send.at[0], recv_sem=recv.at[target - block - 1],
            device_id={"ctx": target}, device_id_type=MESH)

    def arrived(ref, recv, block):
        pltpu.make_async_remote_copy(
            src_ref=ref.at[block], dst_ref=ref.at[block],
            send_sem=kv_send.at[0], recv_sem=recv.at[me - block - 1],
            device_id={"ctx": partner}, device_id_type=MESH).wait_recv()

    last_near = jnp.minimum(chip + near, chips - 1)

    relayed = ((chip == 1) & (core == 1)).astype(jnp.int32)
    bearer = (chip == 3) & (core == 1)

    def own_targets(act):
        def one(c, carry):
            act(c * 2 + core)
            return carry

        if detour:
            lax.fori_loop(chip + 1, last_near + 1 - 2 * relayed, one, 0)

            @pl.when(relayed == 1)
            def _():
                act(me + 4)
        else:
            lax.fori_loop(chip + 1, last_near + 1, one, 0)

        @pl.when(core == 0)
        def _():
            act(partner)

        @pl.when((core == 1) & (chip + near + 1 < chips))
        def _():
            act(me + gap)

    own_targets(lambda d: block_copy(kb, k_recv, kv_send, me, d).start())

    half = STEPS // 2
    for c in range(half):
        rows_copy(w_value, wv, wv_sem, c).wait()
        for i in range(STEPS // half):
            product = jnp.dot(
                tok[c * (STEPS // half) + i], wv[c, i * step_rows:(i + 1) * step_rows, :],
                preferred_element_type=jnp.float32)
            v_acc[...] = product if c == 0 and i == 0 else v_acc[...] + product
    for h in range(kv_heads):
        vb[me, h * HD:(h + 1) * HD, :] = v_acc[:, h * HD:(h + 1) * HD].T.astype(jnp.bfloat16)
    own_targets(lambda d: block_copy(vb, v_recv, kv_send, me, d).start())

    for c in range(STEPS):
        rows_copy(w_query, wq, wq_sem, c).wait()
        if c == STEPS - 1:
            for k in range(n_head):
                wo_copy(owner_of(k)).start()
        product = jnp.dot(tok[c], wq[c], preferred_element_type=jnp.float32)
        q_acc[...] = product if c == 0 else q_acc[...] + product
    for h in range(heads):
        g = h % group
        q[h // group, g * rows:(g + 1) * rows, :] = rotated(q_acc[:, h * HD:(h + 1) * HD])

    def attend(js, own, ready=None):
        doc_row = doc[...].astype(jnp.float32)
        biases = []
        for i, j in enumerate(js):
            column = kb[j, kv_heads * rows:kv_heads * rows + 1, :].astype(jnp.float32)
            ok = jnp.broadcast_to(column, (rows, rows)).T == doc_row
            if own and i == 0:
                ok = ok & (lax.broadcasted_iota(jnp.int32, (rows, rows), 0)
                           <= lax.broadcasted_iota(jnp.int32, (rows, rows), 1))
            bias = jnp.where(ok, 0.0, -1e30).astype(jnp.float32)
            biases.append(jnp.concatenate([bias] * group, axis=1))
        scores = [
            [bias + lax.dot_general(
                kb[j, h * rows:(h + 1) * rows, :], q[h],
                (((1,), (1,)), ((), ())), preferred_element_type=jnp.float32)
             for j, bias in zip(js, biases)]
            for h in range(kv_heads)]
        scales, weights = [], []
        for h in range(kv_heads):
            high = jnp.max(functools.reduce(jnp.maximum, scores[h]), axis=0, keepdims=True)
            if not own:
                high = jnp.maximum(top[h], high)
                scales.append(jnp.exp2((top[h] - high) * FACTOR))
            ps = [jnp.exp2((s - high) * FACTOR) for s in scores[h]]
            total = jnp.sum(functools.reduce(jnp.add, ps), axis=0, keepdims=True)
            top[h] = high
            tot[h] = total if own else tot[h] * scales[h] + total
            weights.append(jnp.concatenate([p.astype(jnp.bfloat16) for p in ps], axis=0))
        if ready is not None:
            ready()
        for h in range(kv_heads):
            mixed = jnp.dot(
                jnp.concatenate([vb[j, h * HD:(h + 1) * HD, :] for j in js], axis=1),
                weights[h], preferred_element_type=jnp.float32)
            acc[h] = mixed if own else acc[h] * scales[h] + mixed

    def keys_in(j):
        arrived(kb, k_recv, j)

    def values_in(j):
        arrived(vb, v_recv, j)

    def pass_on_block(ref, recv, j, relays):
        block_copy(ref, recv, kv_fwd, j, partner).start()
        if relays:
            @pl.when(bearer)
            def _():
                block_copy(ref, recv, kv_fwd, j, me - 2).start()

    def keys_on(j, relays=False):
        keys_in(j)
        pass_on_block(kb, k_recv, j, relays)

    def values_on(j, relays=False):
        values_in(j)
        pass_on_block(vb, v_recv, j, relays)

    @pl.when(core == 0)
    def _():
        attend([me], True)

    @pl.when(core == 1)
    def _():
        keys_in(me - 1)
        attend([me, me - 1], True, lambda: values_in(me - 1))

    count = jnp.minimum(chip, near)

    def mine_of(i):
        return (chip - count + i) * 2 + core

    def other_of(i):
        return (chip - count + i) * 2 + 1 - core

    def chip_step(i, carry):
        mine, other = mine_of(i), other_of(i)
        keys_on(mine)
        attend([mine], False, lambda: values_on(mine))
        keys_in(other)
        attend([other], False, lambda: values_in(other))
        return carry

    def far_step(js):
        for j in js:
            keys_in(j)

        def ready():
            for j in js:
                values_in(j)

        attend(js, False, ready)

    if near == 2:
        @pl.when(chip <= near)
        def _():
            lax.fori_loop(0, count, chip_step, 0)

        @pl.when(chip > near)
        def _():
            mine, other = [mine_of(0), mine_of(1)], [other_of(0), other_of(1)]
            for i, j in enumerate(mine):
                keys_on(j, detour and i == 0)

            def ready():
                for i, j in enumerate(mine):
                    values_on(j, detour and i == 0)

            attend(mine, False, ready)

            @pl.when(core == 0)
            def _():
                far_step(other + [me - gap])

            @pl.when(core == 1)
            def _():
                far_step(other)
    else:
        lax.fori_loop(0, count, chip_step, 0)

        @pl.when((core == 0) & (chip > near))
        def _():
            far_step([me - gap])

    for h in range(kv_heads):
        result = acc[h] * (1.0 / tot[h])
        for g in range(group):
            att[:, (h * group + g) * HD:(h * group + g + 1) * HD] = (
                result[:, g * rows:(g + 1) * rows].T.astype(jnp.bfloat16))

    def piece_copy(p, way, source=None, ctx=None):
        target = z + 1 if way == 0 else z - 1
        slot = p - SUB * target if way == 0 else SUB * (n_head - target) + p
        return pltpu.make_async_remote_copy(
            src_ref=part.at[p] if source is None else source, dst_ref=rbuf.at[way, p],
            send_sem=part_send.at[0], recv_sem=part_recv.at[slot],
            device_id={"head": target} if ctx is None else {"ctx": ctx, "head": target},
            device_id_type=MESH)

    def side_copy(p, i, ctx):
        return pltpu.make_async_remote_copy(
            src_ref=part.at[p], dst_ref=side.at[i],
            send_sem=part_send.at[0], recv_sem=side_recv.at[i],
            device_id={"ctx": ctx}, device_id_type=MESH)

    def piece_arrived(p, way):
        slot = p - SUB * z if way == 0 else SUB * (n_head - z) + p
        pltpu.make_async_remote_copy(
            src_ref=part.at[p], dst_ref=rbuf.at[way, p],
            send_sem=part_send.at[0], recv_sem=part_recv.at[slot],
            device_id={"ctx": partner}, device_id_type=MESH).wait_recv()

    def project(k, carry):
        t = owner_of(k)
        wo_copy(t).wait()
        for s in range(SUB):
            p = t * SUB + s
            if s % WIDE == 0:
                product = jnp.dot(
                    att[...], wo[t, :, s * piece:(s + WIDE) * piece],
                    preferred_element_type=jnp.float32).astype(jnp.bfloat16)
                for i in range(WIDE):
                    part[p + i] = product[:, i * piece:(i + 1) * piece]

            def send(way, t=t, p=p, s=s):
                if not detour:
                    piece_copy(p, way).start()
                    return
                given = giver & (t == (2 if way == 0 else n_head - 3)) & (s >= SUB - SIDE)
                held = helper & (t == (1 if way == 0 else n_head - 2))

                @pl.when(jnp.logical_not(given | held))
                def _():
                    piece_copy(p, way).start()

                if s >= SUB - SIDE:
                    @pl.when(given)
                    def _():
                        side_copy(p, s - SUB + SIDE, me - n_ctx // 2).start()

            @pl.when((z == 0) & (t > 0))
            def _(send=send):
                send(0)

            @pl.when((z == n_head - 1) & (t < n_head - 1))
            def _(send=send):
                send(1)
        return carry

    lax.fori_loop(0, n_head, project, 0)

    if detour:
        for edge, way, t, own in ((0, 0, 2, 1), (n_head - 1, 1, n_head - 3, n_head - 2)):
            @pl.when(helper & (z == edge))
            def _(way=way, t=t, own=own):
                for i in range(SIDE):
                    p = t * SUB + SUB - SIDE + i
                    side_copy(p, i, partner).wait_recv()
                    piece_copy(p, way, side.at[i], me + n_ctx // 2).start()
                for i in range(SUB):
                    piece_copy(own * SUB + i, way).start()

    def pass_on(p, way):
        piece_arrived(p, way)
        part[p] = (part[p].astype(jnp.float32) + rbuf[way, p].astype(jnp.float32)).astype(jnp.bfloat16)
        piece_copy(p, way).start()

    def relay(t, carry):
        a = t - (SUB - 1) * z
        b = t - (SUB - 1) * (n_head - 1 - z)

        @pl.when((z > 0) & (a >= 0) & (a < SUB * (n_head - 1 - z)))
        def _():
            pass_on((n_head - 1 - a // SUB) * SUB + lax.rem(a, SUB), 0)

        @pl.when((z < n_head - 1) & (b >= 0) & (b < SUB * z))
        def _():
            pass_on(b, 1)
        return carry

    @pl.when((z > 0) & (z < n_head - 1))
    def _():
        lax.fori_loop(0, (2 * SUB - 1) * (n_head - 1), relay, 0)

    def last(s, add_left, add_right):
        p = z * SUB + s
        value = part[p].astype(jnp.float32)
        if add_left:
            piece_arrived(p, 0)
            value += rbuf[0, p].astype(jnp.float32)
        if add_right:
            piece_arrived(p, 1)
            value += rbuf[1, p].astype(jnp.float32)
        out[:, s * piece:(s + 1) * piece] = value.astype(jnp.bfloat16)

    own_targets(lambda d: block_copy(kb, k_recv, kv_send, me, d).wait_send())
    own_targets(lambda d: block_copy(vb, v_recv, kv_send, me, d).wait_send())

    def drain_forward(i, carry):
        block_copy(kb, k_recv, kv_fwd, mine_of(i), partner).wait_send()
        block_copy(vb, v_recv, kv_fwd, mine_of(i), partner).wait_send()
        return carry

    lax.fori_loop(0, count, drain_forward, 0)
    if detour:
        @pl.when(bearer)
        def _():
            drain_forward(0, 0)

    for which, left, right in ((z == 0, False, True), (z == n_head - 1, True, False),
                               ((z > 0) & (z < n_head - 1), True, True)):
        @pl.when(which)
        def _(left=left, right=right):
            for s in range(SUB):
                last(s, left, right)

    def drain_piece(p, carry):
        @pl.when((p < z * SUB) | (p >= (z + 1) * SUB))
        def _():
            pltpu.make_async_remote_copy(
                src_ref=part.at[p], dst_ref=rbuf.at[0, p],
                send_sem=part_send.at[0], recv_sem=part_recv.at[0],
                device_id={"ctx": partner}, device_id_type=MESH).wait_send()
        return carry

    lax.fori_loop(0, n_head * SUB, drain_piece, 0)

    if detour:
        @pl.when(helper & ((z == 0) | (z == n_head - 1)))
        def _():
            for i in range(SIDE):
                side_copy(0, i, partner).wait_send()


def solution(mesh):
    n_ctx, n_head = mesh.shape["ctx"], mesh.shape["head"]
    reach = n_ctx // 2 + 1

    def step(tokens, w_query, w_key, w_value, w_out, doc_ids):
        rows, width = tokens.shape
        q_width, kv_width = w_query.shape[1], w_key.shape[1]
        kv_heads, heads = kv_width // HD, q_width // HD
        group = heads // kv_heads
        step_rows = width // STEPS
        out_width = w_out.shape[1]
        pieces = n_head * SUB
        piece = out_width // pieces
        bf16, f32 = jnp.bfloat16, jnp.float32
        dma = pltpu.SemaphoreType.DMA
        return pl.pallas_call(
            functools.partial(kernel, n_ctx, n_head, reach),
            out_shape=pltpu.VMEM((rows, out_width // n_head), bf16),
            in_specs=[pl.BlockSpec(memory_space=pl.ANY)] * 6,
            out_specs=pl.BlockSpec(memory_space=pltpu.VMEM),
            scratch_shapes=[
                pltpu.VMEM((STEPS, rows, step_rows), bf16),
                pltpu.VMEM((STEPS, step_rows, q_width), bf16),
                pltpu.VMEM((STEPS, step_rows, kv_width), bf16),
                pltpu.VMEM((STEPS // 2, 2 * step_rows, kv_width), bf16),
                pltpu.VMEM((n_head, q_width, SUB * piece), bf16),
                pltpu.VMEM((1, rows), jnp.int32),
                pltpu.VMEM((n_ctx, kv_heads * rows + TAIL, HD), bf16),
                pltpu.VMEM((n_ctx, kv_width, rows), bf16),
                pltpu.VMEM((rows, q_width), f32),
                pltpu.VMEM((rows, kv_width), f32),
                pltpu.VMEM((rows, kv_width), f32),
                pltpu.VMEM((kv_heads, group * rows, HD), bf16),
                pltpu.VMEM((rows, HD), f32),
                pltpu.VMEM((rows, HD), f32),
                pltpu.VMEM((kv_heads, 1, group * rows), f32),
                pltpu.VMEM((kv_heads, 1, group * rows), f32),
                pltpu.VMEM((kv_heads, HD, group * rows), f32),
                pltpu.VMEM((rows, q_width), bf16),
                pltpu.VMEM((pieces, rows, piece), bf16),
                pltpu.VMEM((2, pieces, rows, piece), bf16),
                pltpu.VMEM((SIDE, rows, piece), bf16),
                dma((STEPS,)), dma((max(STEPS, n_head),)), dma((STEPS // 2,)), dma((1,)),
                dma((1,)), dma((1,)), dma((reach,)), dma((reach,)),
                dma((1,)), dma((SUB * (n_head + 1),)), dma((SIDE,)),
            ],
            compiler_params=pltpu.CompilerParams(
                collective_id=0, has_side_effects=True, vmem_limit_bytes=60 * 1024 * 1024),
            name="attention_layer",
        )(tokens, w_query, w_key, w_value, w_out, doc_ids.reshape(1, rows))

    return jax.shard_map(
        step,
        mesh=mesh,
        in_specs=(
            P("ctx", None),
            P(None, "head"),
            P(None, "head"),
            P(None, "head"),
            P("head", None),
            P("ctx"),
        ),
        out_specs=P("ctx", "head"),
        check_vma=False,
    )
```

```python
import functools
import math

import jax
import jax.numpy as jnp
from jax import lax
from jax.experimental import pallas as pl
from jax.experimental.pallas import tpu as pltpu
from jax.sharding import PartitionSpec as P

HD = 128
BASE = 500000.0
STEPS = 4
SUB = 4
SIDE = 2
WIDTHS = (2, 0, 2, 0)
TAIL = 16
MESH = pl.DeviceIdType.MESH
FACTOR = math.log2(math.e) / math.sqrt(HD)


def kernel(
    n_ctx, n_head, reach,
    tokens, w_query, w_key, w_value, w_out, docs, out,
    tok, wq, wk, wv, wo, doc, kb, vb, q_acc, k_acc, v_acc, q, cos_ref, sin_ref,
    top, tot, acc, att, part, rbuf, side,
    wq_sem, wo_sem, wv_sem, doc_sem,
    kv_send, kv_fwd, k_recv, v_recv, part_send, part_recv, side_recv,
):
    rows = tokens.shape[0]
    kv_heads = w_key.shape[1] // HD
    heads = w_query.shape[1] // HD
    group = heads // kv_heads
    chips = n_ctx // 2
    near = (reach - 1) // 2
    me = lax.axis_index("ctx")
    z = lax.axis_index("head")
    core = lax.rem(me, 2)
    chip = me // 2
    partner = me + 1 - 2 * core
    step_rows = wq.shape[1]
    v_rows = wv.shape[1]
    piece = part.shape[2]

    def tok_copy(c):
        return pltpu.make_async_copy(
            tokens.at[:, c * step_rows:(c + 1) * step_rows], tok.at[c], wq_sem.at[c])

    def rows_copy(src, dst, sem, c):
        size = dst.shape[1]
        return pltpu.make_async_copy(src.at[c * size:(c + 1) * size, :], dst.at[c], sem.at[c])

    def wo_copy(t):
        width = SUB * piece
        return pltpu.make_async_copy(
            w_out.at[:, pl.ds(pl.multiple_of(t * width, width), width)], wo.at[t], wo_sem.at[t])

    def owner_of(k):
        return jnp.where(z < n_head // 2, n_head - 1 - k, k)

    doc_copy = pltpu.make_async_copy(docs, doc, doc_sem.at[0])
    doc_copy.start()
    for c in range(STEPS):
        tok_copy(c).start()
        rows_copy(w_key, wk, wo_sem, c).start()

    barrier = pltpu.get_barrier_semaphore()

    last_near = jnp.minimum(chip + near, chips - 1)

    def greet(c, carry):
        pl.semaphore_signal(
            barrier, inc=1, device_id={"ctx": c * 2 + core}, device_id_type=MESH)
        return carry

    lax.fori_loop(jnp.maximum(chip - near, 0), chip, greet, 0)
    pl.semaphore_signal(barrier, inc=1, device_id={"ctx": partner}, device_id_type=MESH)
    gap = 2 * (near + 1) - 1
    detour = chips == 4 and n_head == 4
    helper, giver = chip == 0, chip == 2
    bearer = (chip == 3) & (core == 1)
    greeted = (last_near - chip + 1 + (z > 0).astype(jnp.int32)
               + (z < n_head - 1).astype(jnp.int32))
    if detour:
        for inner, edge in ((1, 0), (n_head - 2, n_head - 1)):
            @pl.when(giver & (z == inner))
            def _(edge=edge):
                pl.semaphore_signal(
                    barrier, inc=1, device_id={"ctx": me - n_ctx // 2, "head": edge},
                    device_id_type=MESH)

        @pl.when(helper & ((z == 0) | (z == n_head - 1)))
        def _():
            greet(2, 0)

        @pl.when((chip == 2) & (core == 1))
        def _():
            greet(3, 0)

        greeted = greeted + (
            (helper | giver) & ((z == 0) | (z == n_head - 1))).astype(jnp.int32) + (
            bearer.astype(jnp.int32))

    @pl.when((core == 1) & (chip + near + 1 < chips))
    def _():
        pl.semaphore_signal(barrier, inc=1, device_id={"ctx": me + gap}, device_id_type=MESH)

    @pl.when((core == 0) & (chip > near))
    def _():
        pl.semaphore_signal(barrier, inc=1, device_id={"ctx": me - gap}, device_id_type=MESH)

    @pl.when(z > 0)
    def _():
        pl.semaphore_signal(barrier, inc=1, device_id={"head": z - 1}, device_id_type=MESH)

    @pl.when(z < n_head - 1)
    def _():
        pl.semaphore_signal(barrier, inc=1, device_id={"head": z + 1}, device_id_type=MESH)

    index = lax.broadcasted_iota(jnp.int32, (rows, HD), 1)
    freq = jnp.ones((rows, HD), jnp.float32)
    for b in range((HD // 2).bit_length() - 1):
        freq = freq * jnp.where(
            lax.rem(index // (1 << b), 2) == 1, jnp.float32(BASE ** (-2.0 * (1 << b) / HD)), 1.0)
    places = (me * rows + lax.broadcasted_iota(jnp.int32, (rows, HD), 0)).astype(jnp.float32)
    angles = places * freq
    cos_ref[...] = jnp.cos(angles)
    sine = jnp.sin(angles)
    sin_ref[...] = jnp.where(index < HD // 2, -sine, sine)

    rows_copy(w_value, wv, wv_sem, 0).start()

    def rotated(x):
        return (x * cos_ref[...] + pltpu.roll(x, HD // 2, 1) * sin_ref[...]).astype(jnp.bfloat16)

    for c in range(STEPS):
        tok_copy(c).wait()
        rows_copy(w_key, wk, wo_sem, c).wait()
        for i in ((), (0,), (1,), (2, 3))[c]:
            rows_copy(w_query, wq, wq_sem, i).start()
        if c == 0:
            rows_copy(w_value, wv, wv_sem, 1).start()
        product = jnp.dot(tok[c], wk[c], preferred_element_type=jnp.float32)
        k_acc[...] = product if c == 0 else k_acc[...] + product

    doc_copy.wait()
    kb[me, kv_heads * rows:, :] = jnp.broadcast_to(
        doc[...].astype(jnp.float32), (TAIL, rows)).astype(jnp.bfloat16)
    for h in range(kv_heads):
        kb[me, h * rows:(h + 1) * rows, :] = rotated(k_acc[:, h * HD:(h + 1) * HD])

    pl.semaphore_wait(
        barrier,
        greeted + ((core == 1) & (chip + near + 1 < chips)).astype(jnp.int32)
        + ((core == 0) & (chip > near)).astype(jnp.int32))

    def block_copy(ref, recv, send, block, target):
        return pltpu.make_async_remote_copy(
            src_ref=ref.at[block], dst_ref=ref.at[block],
            send_sem=send.at[0], recv_sem=recv.at[target - block - 1],
            device_id={"ctx": target}, device_id_type=MESH)

    def arrived(ref, recv, block):
        pltpu.make_async_remote_copy(
            src_ref=ref.at[block], dst_ref=ref.at[block],
            send_sem=kv_send.at[0], recv_sem=recv.at[me - block - 1],
            device_id={"ctx": partner}, device_id_type=MESH).wait_recv()

    relayed = ((chip == 1) & (core == 1)).astype(jnp.int32)
    def own_targets(act):
        def one(c, carry):
            act(c * 2 + core)
            return carry

        if detour:
            lax.fori_loop(chip + 1, last_near + 1 - 2 * relayed, one, 0)

            @pl.when(relayed == 1)
            def _():
                act(me + 4)
        else:
            lax.fori_loop(chip + 1, last_near + 1, one, 0)

        @pl.when(core == 0)
        def _():
            act(partner)

        @pl.when((core == 1) & (chip + near + 1 < chips))
        def _():
            act(me + gap)

    own_targets(lambda d: block_copy(kb, k_recv, kv_send, me, d).start())

    half = STEPS // 2
    for c in range(half):
        rows_copy(w_value, wv, wv_sem, c).wait()
        for i in range(STEPS // half):
            product = jnp.dot(
                tok[c * (STEPS // half) + i], wv[c, i * step_rows:(i + 1) * step_rows, :],
                preferred_element_type=jnp.float32)
            v_acc[...] = product if c == 0 and i == 0 else v_acc[...] + product
    for h in range(kv_heads):
        vb[me, h * HD:(h + 1) * HD, :] = v_acc[:, h * HD:(h + 1) * HD].T.astype(jnp.bfloat16)
    own_targets(lambda d: block_copy(vb, v_recv, kv_send, me, d).start())

    for c in range(STEPS):
        rows_copy(w_query, wq, wq_sem, c).wait()
        if c == STEPS - 1:
            for k in range(n_head):
                wo_copy(owner_of(k)).start()
        product = jnp.dot(tok[c], wq[c], preferred_element_type=jnp.float32)
        q_acc[...] = product if c == 0 else q_acc[...] + product
    for h in range(heads):
        g = h % group
        q[h // group, g * rows:(g + 1) * rows, :] = rotated(q_acc[:, h * HD:(h + 1) * HD])

    def attend(js, own, ready=None):
        doc_row = doc[...].astype(jnp.float32)
        biases = []
        for i, j in enumerate(js):
            column = kb[j, kv_heads * rows:kv_heads * rows + 1, :].astype(jnp.float32)
            ok = jnp.broadcast_to(column, (rows, rows)).T == doc_row
            if own and i == 0:
                ok = ok & (lax.broadcasted_iota(jnp.int32, (rows, rows), 0)
                           <= lax.broadcasted_iota(jnp.int32, (rows, rows), 1))
            bias = jnp.where(ok, 0.0, -1e30).astype(jnp.float32)
            biases.append(jnp.concatenate([bias] * group, axis=1))
        scores = [
            [bias + lax.dot_general(
                kb[j, h * rows:(h + 1) * rows, :], q[h],
                (((1,), (1,)), ((), ())), preferred_element_type=jnp.float32)
             for j, bias in zip(js, biases)]
            for h in range(kv_heads)]
        scales, weights = [], []
        for h in range(kv_heads):
            high = jnp.max(functools.reduce(jnp.maximum, scores[h]), axis=0, keepdims=True)
            if not own:
                high = jnp.maximum(top[h], high)
                scales.append(jnp.exp2((top[h] - high) * FACTOR))
            ps = [jnp.exp2((s - high) * FACTOR) for s in scores[h]]
            total = jnp.sum(functools.reduce(jnp.add, ps), axis=0, keepdims=True)
            top[h] = high
            tot[h] = total if own else tot[h] * scales[h] + total
            weights.append(jnp.concatenate([p.astype(jnp.bfloat16) for p in ps], axis=0))
        if ready is not None:
            ready()
        for h in range(kv_heads):
            mixed = jnp.dot(
                jnp.concatenate([vb[j, h * HD:(h + 1) * HD, :] for j in js], axis=1),
                weights[h], preferred_element_type=jnp.float32)
            acc[h] = mixed if own else acc[h] * scales[h] + mixed

    def keys_in(j):
        arrived(kb, k_recv, j)

    def values_in(j):
        arrived(vb, v_recv, j)

    def pass_on_block(ref, recv, j, relays):
        block_copy(ref, recv, kv_fwd, j, partner).start()
        if relays:
            @pl.when(bearer)
            def _():
                block_copy(ref, recv, kv_fwd, j, me - 2).start()

    def keys_on(j, relays=False):
        keys_in(j)
        pass_on_block(kb, k_recv, j, relays)

    def values_on(j, relays=False):
        values_in(j)
        pass_on_block(vb, v_recv, j, relays)

    if detour:
        @pl.when(bearer)
        def _():
            keys_on(me - 4, True)

    @pl.when(core == 0)
    def _():
        attend([me], True)

    @pl.when(core == 1)
    def _():
        keys_in(me - 1)
        attend([me, me - 1], True, lambda: values_in(me - 1))

    if detour:
        @pl.when(bearer)
        def _():
            values_on(me - 4, True)

    count = jnp.minimum(chip, near)

    def mine_of(i):
        return (chip - count + i) * 2 + core

    def other_of(i):
        return (chip - count + i) * 2 + 1 - core

    def chip_step(i, carry):
        mine, other = mine_of(i), other_of(i)
        keys_on(mine)
        attend([mine], False, lambda: values_on(mine))
        keys_in(other)
        attend([other], False, lambda: values_in(other))
        return carry

    def far_step(js):
        for j in js:
            keys_in(j)

        def ready():
            for j in js:
                values_in(j)

        attend(js, False, ready)

    if near == 2:
        mine, other = [mine_of(0), mine_of(1)], [other_of(0), other_of(1)]

        @pl.when(chip < near)
        def _():
            lax.fori_loop(0, count, chip_step, 0)

        @pl.when(chip == near)
        def _():
            for j in mine:
                keys_on(j)
                attend([j], False, functools.partial(values_on, j))
            far_step(other)

        @pl.when(chip > near)
        def _():
            if not detour:
                keys_on(mine[0])
            else:
                @pl.when(core == 0)
                def _():
                    keys_on(mine[0])

            keys_on(mine[1])

            def ready():
                if not detour:
                    values_on(mine[0])
                else:
                    @pl.when(core == 0)
                    def _():
                        values_on(mine[0])

                values_on(mine[1])

            attend(mine, False, ready)

            @pl.when(core == 0)
            def _():
                far_step(other + [me - gap])

            @pl.when(core == 1)
            def _():
                far_step(other)
    else:
        lax.fori_loop(0, count, chip_step, 0)

        @pl.when((core == 0) & (chip > near))
        def _():
            far_step([me - gap])

    for h in range(kv_heads):
        result = acc[h] * (1.0 / tot[h])
        for g in range(group):
            att[:, (h * group + g) * HD:(h * group + g + 1) * HD] = (
                result[:, g * rows:(g + 1) * rows].T.astype(jnp.bfloat16))

    def piece_copy(p, way, source=None, ctx=None):
        target = z + 1 if way == 0 else z - 1
        slot = p - SUB * target if way == 0 else SUB * (n_head - target) + p
        return pltpu.make_async_remote_copy(
            src_ref=part.at[p] if source is None else source, dst_ref=rbuf.at[way, p],
            send_sem=part_send.at[0], recv_sem=part_recv.at[slot],
            device_id={"head": target} if ctx is None else {"ctx": ctx, "head": target},
            device_id_type=MESH)

    def side_copy(p, i, ctx):
        return pltpu.make_async_remote_copy(
            src_ref=part.at[p], dst_ref=side.at[i],
            send_sem=part_send.at[0], recv_sem=side_recv.at[i],
            device_id={"ctx": ctx}, device_id_type=MESH)

    def piece_arrived(p, way):
        slot = p - SUB * z if way == 0 else SUB * (n_head - z) + p
        pltpu.make_async_remote_copy(
            src_ref=part.at[p], dst_ref=rbuf.at[way, p],
            send_sem=part_send.at[0], recv_sem=part_recv.at[slot],
            device_id={"ctx": partner}, device_id_type=MESH).wait_recv()

    def project(k, carry):
        t = owner_of(k)
        wo_copy(t).wait()
        for s in range(SUB):
            p = t * SUB + s
            wide = WIDTHS[s]
            if wide:
                product = jnp.dot(
                    att[...], wo[t, :, s * piece:(s + wide) * piece],
                    preferred_element_type=jnp.float32).astype(jnp.bfloat16)
                for i in range(wide):
                    part[p + i] = product[:, i * piece:(i + 1) * piece]

            def send(way, t=t, p=p, s=s):
                if not detour:
                    piece_copy(p, way).start()
                    return
                given = giver & (t == (2 if way == 0 else n_head - 3)) & (s >= SUB - SIDE)
                held = helper & (t == (1 if way == 0 else n_head - 2))

                @pl.when(jnp.logical_not(given | held))
                def _():
                    piece_copy(p, way).start()

                if s >= SUB - SIDE:
                    @pl.when(given)
                    def _():
                        side_copy(p, s - SUB + SIDE, me - n_ctx // 2).start()

            @pl.when((z == 0) & (t > 0))
            def _(send=send):
                send(0)

            @pl.when((z == n_head - 1) & (t < n_head - 1))
            def _(send=send):
                send(1)
        return carry

    lax.fori_loop(0, n_head, project, 0)

    if detour:
        for edge, way, t, own in ((0, 0, 2, 1), (n_head - 1, 1, n_head - 3, n_head - 2)):
            @pl.when(helper & (z == edge))
            def _(way=way, t=t, own=own):
                for i in range(SIDE):
                    p = t * SUB + SUB - SIDE + i
                    side_copy(p, i, partner).wait_recv()
                    piece_copy(p, way, side.at[i], me + n_ctx // 2).start()
                for i in range(SUB):
                    piece_copy(own * SUB + i, way).start()

    def pass_on(p, way):
        piece_arrived(p, way)
        part[p] = (part[p].astype(jnp.float32) + rbuf[way, p].astype(jnp.float32)).astype(jnp.bfloat16)
        piece_copy(p, way).start()

    def relay(t, carry):
        a = t - (SUB - 1) * z
        b = t - (SUB - 1) * (n_head - 1 - z)

        def up():
            pass_on((n_head - 1 - a // SUB) * SUB + lax.rem(a, SUB), 0)

        upward = (a >= 0) & (a < SUB * (n_head - 1 - z))
        pl.when((z < n_head // 2) & upward)(up)

        @pl.when((b >= 0) & (b < SUB * z))
        def _():
            pass_on(b, 1)

        pl.when((z >= n_head // 2) & upward)(up)
        return carry

    @pl.when((z > 0) & (z < n_head - 1))
    def _():
        lax.fori_loop(0, (2 * SUB - 1) * (n_head - 1), relay, 0)

    def last(s, add_left, add_right):
        p = z * SUB + s
        value = part[p].astype(jnp.float32)
        if add_left:
            piece_arrived(p, 0)
            value += rbuf[0, p].astype(jnp.float32)
        if add_right:
            piece_arrived(p, 1)
            value += rbuf[1, p].astype(jnp.float32)
        out[:, s * piece:(s + 1) * piece] = value.astype(jnp.bfloat16)

    own_targets(lambda d: block_copy(kb, k_recv, kv_send, me, d).wait_send())
    own_targets(lambda d: block_copy(vb, v_recv, kv_send, me, d).wait_send())

    def drain_forward(i, carry):
        block_copy(kb, k_recv, kv_fwd, mine_of(i), partner).wait_send()
        block_copy(vb, v_recv, kv_fwd, mine_of(i), partner).wait_send()
        return carry

    lax.fori_loop(0, count, drain_forward, 0)
    if detour:
        @pl.when(bearer)
        def _():
            drain_forward(0, 0)

    for which, left, right in ((z == 0, False, True), (z == n_head - 1, True, False),
                               ((z > 0) & (z < n_head - 1), True, True)):
        @pl.when(which)
        def _(left=left, right=right):
            for s in range(SUB):
                last(s, left, right)

    def drain_piece(p, carry):
        @pl.when((p < z * SUB) | (p >= (z + 1) * SUB))
        def _():
            pltpu.make_async_remote_copy(
                src_ref=part.at[p], dst_ref=rbuf.at[0, p],
                send_sem=part_send.at[0], recv_sem=part_recv.at[0],
                device_id={"ctx": partner}, device_id_type=MESH).wait_send()
        return carry

    lax.fori_loop(0, n_head * SUB, drain_piece, 0)

    if detour:
        @pl.when(helper & ((z == 0) | (z == n_head - 1)))
        def _():
            for i in range(SIDE):
                side_copy(0, i, partner).wait_send()


def solution(mesh):
    n_ctx, n_head = mesh.shape["ctx"], mesh.shape["head"]
    reach = n_ctx // 2 + 1

    def step(tokens, w_query, w_key, w_value, w_out, doc_ids):
        rows, width = tokens.shape
        q_width, kv_width = w_query.shape[1], w_key.shape[1]
        kv_heads, heads = kv_width // HD, q_width // HD
        group = heads // kv_heads
        step_rows = width // STEPS
        out_width = w_out.shape[1]
        pieces = n_head * SUB
        piece = out_width // pieces
        bf16, f32 = jnp.bfloat16, jnp.float32
        dma = pltpu.SemaphoreType.DMA
        return pl.pallas_call(
            functools.partial(kernel, n_ctx, n_head, reach),
            out_shape=pltpu.VMEM((rows, out_width // n_head), bf16),
            in_specs=[pl.BlockSpec(memory_space=pl.ANY)] * 6,
            out_specs=pl.BlockSpec(memory_space=pltpu.VMEM),
            scratch_shapes=[
                pltpu.VMEM((STEPS, rows, step_rows), bf16),
                pltpu.VMEM((STEPS, step_rows, q_width), bf16),
                pltpu.VMEM((STEPS, step_rows, kv_width), bf16),
                pltpu.VMEM((STEPS // 2, 2 * step_rows, kv_width), bf16),
                pltpu.VMEM((n_head, q_width, SUB * piece), bf16),
                pltpu.VMEM((1, rows), jnp.int32),
                pltpu.VMEM((n_ctx, kv_heads * rows + TAIL, HD), bf16),
                pltpu.VMEM((n_ctx, kv_width, rows), bf16),
                pltpu.VMEM((rows, q_width), f32),
                pltpu.VMEM((rows, kv_width), f32),
                pltpu.VMEM((rows, kv_width), f32),
                pltpu.VMEM((kv_heads, group * rows, HD), bf16),
                pltpu.VMEM((rows, HD), f32),
                pltpu.VMEM((rows, HD), f32),
                pltpu.VMEM((kv_heads, 1, group * rows), f32),
                pltpu.VMEM((kv_heads, 1, group * rows), f32),
                pltpu.VMEM((kv_heads, HD, group * rows), f32),
                pltpu.VMEM((rows, q_width), bf16),
                pltpu.VMEM((pieces, rows, piece), bf16),
                pltpu.VMEM((2, pieces, rows, piece), bf16),
                pltpu.VMEM((SIDE, rows, piece), bf16),
                dma((STEPS,)), dma((max(STEPS, n_head),)), dma((STEPS // 2,)), dma((1,)),
                dma((1,)), dma((1,)), dma((reach,)), dma((reach,)),
                dma((1,)), dma((SUB * (n_head + 1),)), dma((SIDE,)),
            ],
            compiler_params=pltpu.CompilerParams(
                collective_id=0, has_side_effects=True, vmem_limit_bytes=60 * 1024 * 1024),
            name="attention_layer",
        )(tokens, w_query, w_key, w_value, w_out, doc_ids.reshape(1, rows))

    return jax.shard_map(
        step,
        mesh=mesh,
        in_specs=(
            P("ctx", None),
            P(None, "head"),
            P(None, "head"),
            P(None, "head"),
            P("head", None),
            P("ctx"),
        ),
        out_specs=P("ctx", "head"),
        check_vma=False,
    )
```
